32 devices in a mesh: wide: 8 (over y, x, core), narrow: 4 (over z).
Axes of the slice: x: 2, y: 2, z: 4, core: 2. Of those that a mesh axis runs over, the one named last changes fastest.
Arguments:
- coefficients: float32 [8, 8192, 8192], P(None, 'wide', 'narrow'), may hold values from -0.07 to 0.07
- tensor_blocks: float32 [8, 32, 8192], P(None, 'wide', 'narrow'), may hold values from -6 to 6
- basis_rows: float32 [32, 8192], P(None, ('wide', 'narrow')), may hold values from -1.1 to 1.1, as said below
Outputs:
- new_basis: float32 [32, 8192], P(None, ('wide', 'narrow'))
- projection: float32 [32, 32], replicated
- factor: float32 [32, 32], replicated
The draws below stay inside these ranges and needn't reach their ends.
Inputs may be any that keep to these rules, and one draw needn't show every extreme that they name: The rows of basis_rows are nearly but not exactly orthonormal: basis_rows basis_rows^T differs from the identity by less than 0.2 in spectral norm.
All inputs are finite; a program needn't handle non-finite values.
Results may differ from the reference program's by a relative error of at most 0.0002.
Values sent between devices are 32-bit elements; how exact they have to be, the bound alone decides.
A program may use at most 128 MiB of HBM per device.

```python
import math
import jax
import jax.numpy as jnp
from jax import lax

N = 8192
K = 8
R = 32
M = 32


def orthonormal_rows(raw):
    hi = lax.Precision.HIGHEST
    for sweep in range(2):
        gram = jnp.dot(raw, raw.T, precision=hi)
        lower = jnp.linalg.cholesky(gram)
        raw = lax.linalg.triangular_solve(lower, raw, left_side=True, lower=True)
    return raw


def coefficient_values(key):
    spread = 0.5 / math.sqrt(K * N)
    inner_key = jax.random.fold_in(key, 11)
    values = jnp.clip(jax.random.normal(inner_key, (K, N, N), jnp.float32), -6.0, 6.0) * spread
    return values


def tensor_values(key):
    inner_key = jax.random.fold_in(key, 12)
    values = jnp.clip(jax.random.normal(inner_key, (K, R, N), jnp.float32), -6.0, 6.0)
    return values


def draw_coefficients(key, part):
    return coefficient_values(key).astype(jnp.float32)


def draw_tensor_blocks(key, part):
    return tensor_values(key).astype(jnp.float32)


def draw_basis_rows(key, part):
    hi = lax.Precision.HIGHEST
    image = jnp.einsum('kic,krc->ir', tensor_values(key), coefficient_values(key), precision=hi)
    noise_key = jax.random.fold_in(key, 13)
    turn_key = jax.random.fold_in(key, 14)
    noise = jax.random.normal(noise_key, (M, N), jnp.float32)
    tilt = 0.06
    frame = orthonormal_rows(image[:M] + 0.1 * noise)
    turn = orthonormal_rows(jax.random.normal(turn_key, (M, M), jnp.float32))
    mixer = jnp.eye(M, dtype=jnp.float32) + tilt * turn
    return jnp.dot(mixer, frame, precision=hi).astype(jnp.float32)


def setup_inputs(seed: int = 0) -> dict:
    seeds = jax.random.split(jax.random.key(seed), 4)
    return {
        "coefficients": draw_coefficients(jax.random.fold_in(seeds[3], 71), 0),
        "tensor_blocks": draw_tensor_blocks(jax.random.fold_in(seeds[3], 71), 0),
        "basis_rows": draw_basis_rows(jax.random.fold_in(seeds[3], 71), 0),
    }


def reference(coefficients, tensor_blocks, basis_rows):
    hi = lax.Precision.HIGHEST
    image = jnp.einsum('kic,krc->ir', tensor_blocks, coefficients, precision=hi)
    first = jnp.dot(basis_rows, image.T, precision=hi)
    once = image - jnp.dot(first.T, basis_rows, precision=hi)
    second = jnp.dot(basis_rows, once.T, precision=hi)
    twice = once - jnp.dot(second.T, basis_rows, precision=hi)
    gram = jnp.dot(twice, twice.T, precision=hi) / N
    factor = jnp.linalg.cholesky(gram)
    new_basis = lax.linalg.triangular_solve(factor, twice, left_side=True, lower=True)
    return (new_basis, first + second, factor)
```

```python
import functools

import jax
import jax.numpy as jnp
from jax import lax
from jax.experimental import pallas as pl
from jax.experimental.pallas import tpu as pltpu
from jax.sharding import PartitionSpec as P

MESH = pl.DeviceIdType.MESH
HI = lax.Precision.HIGHEST
F32 = jnp.float32
BF16 = jnp.bfloat16
DEPTH = 5
PANEL = 8
LANES = 128
TILE = 256
GROUP = 4
NT = (((1,), (1,)), ((), ()))
NN = (((1,), (0,)), ((), ()))


def nt(a, b):
    return lax.dot_general(a, b, NT, precision=HI, preferred_element_type=F32)


def nn(a, b):
    return lax.dot_general(a, b, NN, precision=HI, preferred_element_type=F32)


def fold(r, c):
    return 128 // c if 128 % c == 0 and r % (128 // c) == 0 else 1


def pack(x, f):
    r = x.shape[0] // f
    return jnp.concatenate([x[q * r:(q + 1) * r] for q in range(f)], axis=1)


def unpack(x, f):
    c = x.shape[1] // f
    return jnp.concatenate([x[:, q * c:(q + 1) * c] for q in range(f)], axis=0)


def packed(r, c):
    f = fold(r, c)
    return (r // f, c * f)


def split(x):
    hi = x.astype(BF16)
    return hi, (x - hi.astype(F32)).astype(BF16)


def each(lo, hi, f):
    if hi - lo <= 8:
        for d in range(lo, hi):
            f(d)
    else:
        pl.loop(lo, hi)(f)


def widen(x, width):
    return x[:, :width] if width <= LANES else jnp.concatenate([x] * (width // LANES), axis=1)


def factor_solve(a, x):
    ranks, rows = x.shape
    sub = lax.broadcasted_iota(jnp.int32, (ranks, LANES), 0)
    r_i = lax.broadcasted_iota(jnp.int32, (ranks, ranks), 0)
    c_i = lax.broadcasted_iota(jnp.int32, (ranks, ranks), 1)
    scale = jnp.ones((ranks, LANES), F32)
    lower = jnp.zeros((ranks, ranks), F32)
    panel = PANEL if ranks % PANEL == 0 else 1
    for b0 in range(0, ranks, panel):
        cols = [jnp.broadcast_to(a[:, b0 + t:b0 + t + 1], (ranks, LANES)) for t in range(panel)]
        for t in range(panel):
            j = b0 + t
            rs = lax.rsqrt(cols[t][j:j + 1, :])
            full = cols[t] * rs
            lower = jnp.where((c_i == j) & (r_i >= j), full[:, :ranks], lower)
            below = jnp.where(sub > j, full, 0.0)
            scale = jnp.where(sub == j, rs, scale)
            for u in range(t + 1, panel):
                cols[u] = cols[u] - below * below[b0 + u:b0 + u + 1, :]
            if j + 1 < ranks:
                a = a - below[:, :ranks] * (a[j:j + 1, :] * rs[:, :ranks])
                x = x - widen(below, rows) * (x[j:j + 1, :] * widen(rs, rows))
    return x * widen(scale, rows), lower


def kernel(wide, narrow, coef, tens, basis, out_image, out_sums, out_hm,
           buf, own_buf, tg, tf, ts, tt, acc, low, me_ref, part, img, sums, hm, azc, awc, azs, aws,
           csem, osem, lsem, xsem, t_send, t_recv, r_send, r_recv, c_sem, s_sem):
    w = lax.axis_index("wide")
    n = lax.axis_index("narrow")
    terms, own, cols = tens.shape
    ranks = own * wide
    m, rows = basis.shape
    half = wide // 2
    depth = min(DEPTH, terms)
    away = narrow - 1
    tile = TILE if cols % TILE == 0 else cols
    group = GROUP if terms % GROUP == 0 else 1
    sib = w + 1 - 2 * lax.rem(w, 2)

    def peer(d):
        return lax.rem(w + 2 * d, wide)

    def zpeer(d):
        return lax.rem(n + d, narrow)

    def remote(src, dst, ss, rs, dev):
        return pltpu.make_async_remote_copy(
            src_ref=src, dst_ref=dst, send_sem=ss, recv_sem=rs, device_id=dev, device_id_type=MESH)

    def block(j):
        return lax.rem(n + 1 + j, narrow)

    def source(k, j):
        r0 = pl.multiple_of(block(j) * rows, rows)
        return coef.at[k, pl.ds(r0, rows), :]

    def fetch(k):
        for j in range(away):
            pltpu.make_async_copy(source(k, j), buf.at[k % depth, j], csem.at[k % depth]).start()

    def load(k, lo, count):
        dst = buf.at[k % depth, pl.ds(lo, count)]
        return pltpu.make_async_copy(dst, dst, csem.at[k % depth])

    def fetch_own(k):
        pltpu.make_async_copy(source(k, away), own_buf.at[k], osem.at[k // group]).start()

    def load_own(g):
        dst = own_buf.at[pl.ds(g * group, group)]
        return pltpu.make_async_copy(dst, dst, osem.at[g])

    local_t = pltpu.make_async_copy(tens, tg.at[:, w], lsem.at[0])
    local_b = pltpu.make_async_copy(basis, me_ref, lsem.at[1])
    local_t.start()
    local_b.start()

    barrier = pltpu.get_barrier_semaphore()

    @pl.loop(1, wide)
    def _(d):
        pl.semaphore_signal(barrier, inc=1, device_id=(lax.rem(w + d, wide), n), device_id_type=MESH)

    for d in range(1, narrow):
        pl.semaphore_signal(barrier, inc=1, device_id=(w, zpeer(d)), device_id_type=MESH)
    local_t.wait()
    local_b.wait()
    for k in range(depth):
        fetch(k)
    me = me_ref[...]
    azc[n] = pack(nt(me, me), fold(m, m))
    pl.semaphore_wait(barrier, wide - 1 + narrow - 1)

    def t_out(k, d):
        return remote(tg.at[k, w], tg.at[k, w], t_send, t_recv.at[k, 0], (peer(d), n))

    def t_sib(k):
        return remote(tg.at[k, w], tg.at[k, w], t_send, t_recv.at[k, 1], (sib, n))

    def t_fwd(k, d):
        p = peer(d)
        return remote(tg.at[k, p], tg.at[k, p], t_send, t_recv.at[k, 1], (sib, n))

    def t_in(k, i, count):
        some = tg.at[k, pl.ds(0, count)]
        remote(some, some, t_send, t_recv.at[k, i], (sib, n)).wait_recv()

    @pl.loop(0, terms)
    def _(k):
        each(1, half, lambda d: t_out(k, d).start())
        t_sib(k).start()

    def forward(k):
        t_in(k, 0, half - 1)
        each(1, half, lambda d: t_fwd(k, d).start())

    def prepare(k):
        t_in(k, 1, half)
        for q in range(wide):
            tf[q * own:(q + 1) * own, :] = tg[k, q]
        hi, lo = split(tf[...])
        ts[k] = hi
        tt[k] = jnp.concatenate([hi, lo], axis=0).T

    def products(work):
        highs, lows = [None] * len(work), [None] * len(work)

        def stream(i, c):
            k, view = work[i]
            hi, _ = split(view[:, c:c + tile])
            p = lax.dot_general(hi, tt[k, c:c + tile, :], NN, preferred_element_type=F32)
            highs[i] = p if c == 0 else highs[i] + p

        def push(i, c):
            k, view = work[i]
            _, lo = split(view[:, c:c + tile])
            q = lax.dot_general(ts[k, :, c:c + tile], lo, NT, preferred_element_type=F32)
            lows[i] = q if c == 0 else lows[i] + q

        for c in range(0, cols, tile):
            for i in range(len(work)):
                push(i, c)
                stream(i, c)
        return highs, lows

    def reducer(az, aw, sems):
        def z_out(d):
            return remote(az.at[n], az.at[n], sems.at[0], sems.at[1], (w, zpeer(d)))

        def w_out(d):
            return remote(aw.at[w], aw.at[w], sems.at[2], sems.at[3], (lax.rem(w + d, wide), n))

        some_z = az.at[pl.ds(0, narrow - 1)]
        some_w = aw.at[pl.ds(0, wide - 1)]
        all_z = remote(some_z, some_z, sems.at[0], sems.at[1], (sib, n))
        all_w = remote(some_w, some_w, sems.at[2], sems.at[3], (sib, n))

        def z_start():
            for d in range(1, narrow):
                z_out(d).start()

        def z_finish():
            all_z.wait_recv()
            t = az[0]
            for q in range(1, narrow):
                t = t + az[q]
            aw[w] = t
            each(1, wide, lambda d: w_out(d).start())

        def w_finish():
            all_w.wait_recv()
            t = aw[0]
            for q in range(1, wide):
                t = t + aw[q]
            return t

        def drain():
            all_z.wait_send()
            all_w.wait_send()

        return z_start, z_finish, w_finish, drain

    c_start, c_mid, c_end, c_drain = reducer(azc, awc, c_sem)
    s_start, s_mid, s_end, s_drain = reducer(azs, aws, s_sem)
    c_start()
    forward(0)
    prepare(0)

    def advance(k, lo, hi):
        load(k, lo, hi - lo).wait()
        highs, lows = products([(k, buf.at[k % depth, j]) for j in range(lo, hi)])
        for j, p, q in zip(range(lo, hi), highs, lows):
            acc[j] = p if k == 0 else acc[j] + p
            low[j] = q if k == 0 else low[j] + q
        if k + depth < terms and hi == away:
            fetch(k + depth)

    for k in range(terms):
        if k == 0:
            advance(0, 0, away)
            if terms > 1:
                forward(1)
        else:
            prepare(k)
            advance(k, 0, away)
        if k + depth == terms:
            for q in range(terms):
                fetch_own(q)
        if k + 2 < terms:
            forward(k + 2)
        if k == 1:
            c_mid()

    def r_out(j):
        return remote(part.at[j], img.at[n], r_send, r_recv, (w, block(j)))

    some_img = img.at[pl.ds(0, away)]
    all_r = remote(part, some_img, r_send, r_recv, (sib, n))

    def settle(high, lows):
        v = high.T
        return v[0:ranks] + v[ranks:2 * ranks] + lows

    for j in range(away):
        part[j] = settle(acc[j], low[j])
        r_out(j).start()

    corr = unpack(c_end(), fold(m, m))
    eye = jnp.where(lax.broadcasted_iota(jnp.int32, (m, m), 0) == lax.broadcasted_iota(jnp.int32, (m, m), 1), 1.0, 0.0)
    e = corr - eye
    e2 = nn(e, e)
    hm[0] = eye - e
    hm[1] = (eye - e) + (e2 - nn(e, e2))
    put_hm = pltpu.make_async_copy(hm, out_hm, xsem.at[0])
    put_hm.start()

    high, lows = None, None
    for g in range(terms // group):
        load_own(g).wait()
        ps, qs = products([(k, own_buf.at[k]) for k in range(g * group, g * group + group)])
        p, q = functools.reduce(jnp.add, ps), functools.reduce(jnp.add, qs)
        high = p if g == 0 else high + p
        lows = q if g == 0 else lows + q

    image = settle(high, lows)
    all_r.wait_recv()
    for d in range(1, narrow):
        image = image + img[zpeer(d)]
    img[n] = image
    put_image = pltpu.make_async_copy(img.at[n], out_image, xsem.at[1])
    put_image.start()
    me = me_ref[...]
    both = nt(image, jnp.concatenate([me, image], axis=0))
    azs[n] = pack(both, fold(ranks, m + ranks))
    s_start()
    c_drain()
    all_r.wait_send()
    sent = tg.at[:, pl.ds(0, wide - 1)]
    remote(sent, sent, t_send, t_recv.at[0, 0], (sib, n)).wait_send()
    put_hm.wait()
    put_image.wait()
    s_mid()
    sums[...] = s_end()
    put_sums = pltpu.make_async_copy(sums, out_sums, xsem.at[2])
    put_sums.start()
    s_drain()
    put_sums.wait()


def finish(total, image_in, sums_in, hm_in, basis_in, new_out, proj_out, fac_out,
           image, sums, hm, me, new, proj, fac, sem):
    ins = [pltpu.make_async_copy(s, d, sem.at[i]) for i, (s, d) in enumerate(
        ((sums_in, sums), (hm_in, hm), (image_in, image), (basis_in, me)))]
    for c in ins:
        c.start()
    for c in ins:
        c.wait()
    m = me.shape[0]
    ranks = image.shape[0]
    both = unpack(sums[...], fold(ranks, m + ranks))
    first_t = both[:, 0:m]
    square = both[:, m:m + ranks]
    proj_t = nn(first_t, hm[0])
    gram = (square - nt(nn(first_t, hm[1]), first_t)) * (1.0 / total)
    proj[...] = nt(hm[0], first_t)
    x, lower = factor_solve(gram, image[...] - nn(proj_t, me[...]))
    new[...] = x
    fac[...] = lower
    outs = [pltpu.make_async_copy(s, d, sem.at[i]) for i, (s, d) in enumerate(
        ((new, new_out), (proj, proj_out), (fac, fac_out)))]
    for c in outs:
        c.start()
    for c in outs:
        c.wait()


def body(wide, narrow, total, coefficients, tensor_blocks, basis_rows):
    terms, own, cols = tensor_blocks.shape
    m, rows = basis_rows.shape
    ranks = own * wide
    depth = min(DEPTH, terms)
    dma = lambda *s: pltpu.SemaphoreType.DMA(s)
    vm = lambda s, t=F32: pltpu.VMEM(s, t)
    shape = lambda *s: jax.ShapeDtypeStruct(s, F32)
    anywhere = pl.BlockSpec(memory_space=pl.ANY)
    cpack, spack = packed(m, m), packed(ranks, m + ranks)
    image, sums, hm = pl.pallas_call(
        functools.partial(kernel, wide, narrow),
        out_shape=(shape(ranks, rows), shape(*spack), shape(2, m, m)),
        in_specs=[anywhere] * 3,
        out_specs=[anywhere] * 3,
        scratch_shapes=[
            vm((depth, narrow - 1, rows, cols)),
            vm((terms, rows, cols)),
            vm((terms, wide, own, cols)),
            vm((ranks, cols)),
            vm((terms, ranks, cols), BF16),
            vm((terms, cols, 2 * ranks), BF16),
            vm((narrow - 1, rows, 2 * ranks)),
            vm((narrow - 1, ranks, rows)),
            vm((m, rows)),
            vm((narrow - 1, ranks, rows)),
            vm((narrow, ranks, rows)),
            vm(spack),
            vm((2, m, m)),
            vm((narrow,) + cpack),
            vm((wide,) + cpack),
            vm((narrow,) + spack),
            vm((wide,) + spack),
            dma(depth), dma(terms), dma(2), dma(3),
            pltpu.SemaphoreType.DMA, dma(terms, 2),
            pltpu.SemaphoreType.DMA, pltpu.SemaphoreType.DMA, dma(4), dma(4),
        ],
        compiler_params=pltpu.CompilerParams(
            collective_id=0, has_side_effects=True, vmem_limit_bytes=62 * 1024 * 1024),
        name="krylov_step",
    )(coefficients, tensor_blocks, basis_rows)
    return pl.pallas_call(
        functools.partial(finish, total),
        out_shape=(shape(ranks, rows), shape(m, ranks), shape(ranks, ranks)),
        in_specs=[anywhere] * 4,
        out_specs=[anywhere] * 3,
        scratch_shapes=[
            vm((ranks, rows)), vm(spack), vm((2, m, m)), vm((m, rows)),
            vm((ranks, rows)), vm((m, ranks)), vm((ranks, ranks)), dma(4),
        ],
        name="krylov_finish",
    )(image, sums, hm, basis_rows)


def solution(mesh):
    wide, narrow = mesh.shape["wide"], mesh.shape["narrow"]
    in_specs = (P(None, "wide", "narrow"), P(None, "wide", "narrow"), P(None, ("wide", "narrow")))
    out_specs = (P(None, ("wide", "narrow")), P(), P())

    def whole(coefficients, tensor_blocks, basis_rows):
        total = coefficients.shape[1]
        return jax.shard_map(functools.partial(body, wide, narrow, total), mesh=mesh,
                             in_specs=in_specs, out_specs=out_specs, check_vma=False)(
            coefficients, tensor_blocks, basis_rows)

    return whole
```

```python
import functools

import jax
import jax.numpy as jnp
from jax import lax
from jax.experimental import pallas as pl
from jax.experimental.pallas import tpu as pltpu
from jax.sharding import PartitionSpec as P

MESH = pl.DeviceIdType.MESH
HI = lax.Precision.HIGHEST
F32 = jnp.float32
BF16 = jnp.bfloat16
DEPTH = 6
PANEL = 8
LANES = 128
TILE = 256
GROUP = 4
NT = (((1,), (1,)), ((), ()))
NN = (((1,), (0,)), ((), ()))


def nt(a, b):
    return lax.dot_general(a, b, NT, precision=HI, preferred_element_type=F32)


def nn(a, b):
    return lax.dot_general(a, b, NN, precision=HI, preferred_element_type=F32)


def fold(r, c):
    return 128 // c if 128 % c == 0 and r % (128 // c) == 0 else 1


def pack(x, f):
    r = x.shape[0] // f
    return jnp.concatenate([x[q * r:(q + 1) * r] for q in range(f)], axis=1)


def unpack(x, f):
    c = x.shape[1] // f
    return jnp.concatenate([x[:, q * c:(q + 1) * c] for q in range(f)], axis=0)


def packed(r, c):
    f = fold(r, c)
    return (r // f, c * f)


def split(x):
    hi = x.astype(BF16)
    return hi, (x - hi.astype(F32)).astype(BF16)


def each(lo, hi, f):
    if hi - lo <= 8:
        for d in range(lo, hi):
            f(d)
    else:
        pl.loop(lo, hi)(f)


def widen(x, width):
    return x[:, :width] if width <= LANES else jnp.concatenate([x] * (width // LANES), axis=1)


def factor_solve(a, x):
    ranks, rows = x.shape
    sub = lax.broadcasted_iota(jnp.int32, (ranks, LANES), 0)
    r_i = lax.broadcasted_iota(jnp.int32, (ranks, ranks), 0)
    c_i = lax.broadcasted_iota(jnp.int32, (ranks, ranks), 1)
    scale = jnp.ones((ranks, LANES), F32)
    lower = jnp.zeros((ranks, ranks), F32)
    panel = PANEL if ranks % PANEL == 0 else 1
    for b0 in range(0, ranks, panel):
        cols = [jnp.broadcast_to(a[:, b0 + t:b0 + t + 1], (ranks, LANES)) for t in range(panel)]
        for t in range(panel):
            j = b0 + t
            rs = lax.rsqrt(cols[t][j:j + 1, :])
            full = cols[t] * rs
            lower = jnp.where((c_i == j) & (r_i >= j), full[:, :ranks], lower)
            below = jnp.where(sub > j, full, 0.0)
            scale = jnp.where(sub == j, rs, scale)
            for u in range(t + 1, panel):
                cols[u] = cols[u] - below * below[b0 + u:b0 + u + 1, :]
            if j + 1 < ranks:
                a = a - below[:, :ranks] * (a[j:j + 1, :] * rs[:, :ranks])
                x = x - widen(below, rows) * (x[j:j + 1, :] * widen(rs, rows))
    return x * widen(scale, rows), lower


def kernel(wide, narrow, coef, tens, basis, out_image, out_sums, out_hm,
           buf, tg, tf, ts, tt, acc, low, me_ref, part, img, azc, awc, azs, aws,
           csem, osem, lsem, t_send, t_recv, r_send, r_recv, c_sem, s_sem):
    w = lax.axis_index("wide")
    n = lax.axis_index("narrow")
    terms, own, cols = tens.shape
    ranks = own * wide
    m, rows = basis.shape
    half = wide // 2
    depth = min(DEPTH, terms)
    away = narrow - 1
    tile = TILE if cols % TILE == 0 else cols
    group = GROUP if terms % GROUP == 0 else 1
    sib = w + 1 - 2 * lax.rem(w, 2)

    def peer(d):
        return lax.rem(w + 2 * d, wide)

    def zpeer(d):
        return lax.rem(n + d, narrow)

    def remote(src, dst, ss, rs, dev):
        return pltpu.make_async_remote_copy(
            src_ref=src, dst_ref=dst, send_sem=ss, recv_sem=rs, device_id=dev, device_id_type=MESH)

    def block(j):
        return lax.rem(n + 1 + j, narrow)

    def source(k, j):
        r0 = pl.multiple_of(block(j) * rows, rows)
        return coef.at[k, pl.ds(r0, rows), :]

    def fetch(k):
        for j in range(away):
            pltpu.make_async_copy(source(k, j), buf.at[k % depth, j], csem.at[k % depth]).start()

    def load(k):
        dst = buf.at[k % depth]
        return pltpu.make_async_copy(dst, dst, csem.at[k % depth])

    def own_view(k):
        return buf.at[(terms - depth + k // away) % depth, k % away]

    def load_own(k):
        return pltpu.make_async_copy(source(k, away), own_view(k), osem.at[k])

    local_t = pltpu.make_async_copy(tens, tg.at[:, w], lsem.at[0])
    local_b = pltpu.make_async_copy(basis, me_ref, lsem.at[1])
    local_t.start()
    local_b.start()

    barrier = pltpu.get_barrier_semaphore()

    @pl.loop(1, wide)
    def _(d):
        pl.semaphore_signal(barrier, inc=1, device_id=(lax.rem(w + d, wide), n), device_id_type=MESH)

    for d in range(1, narrow):
        pl.semaphore_signal(barrier, inc=1, device_id=(w, zpeer(d)), device_id_type=MESH)
    local_t.wait()
    local_b.wait()
    for k in range(depth):
        fetch(k)
    me = me_ref[...]
    azc[n] = pack(nt(me, me), fold(m, m))
    pl.semaphore_wait(barrier, wide - 1 + narrow - 1)

    def t_out(k, d):
        return remote(tg.at[k, w], tg.at[k, w], t_send, t_recv.at[k, 0], (peer(d), n))

    def t_sib(k):
        return remote(tg.at[k, w], tg.at[k, w], t_send, t_recv.at[k, 1], (sib, n))

    def t_fwd(k, d):
        p = peer(d)
        return remote(tg.at[k, p], tg.at[k, p], t_send, t_recv.at[k, 1], (sib, n))

    def t_in(k, i, count):
        some = tg.at[k, pl.ds(0, count)]
        remote(some, some, t_send, t_recv.at[k, i], (sib, n)).wait_recv()

    @pl.loop(0, terms)
    def _(k):
        each(1, half, lambda d: t_out(k, d).start())
        t_sib(k).start()

    def forward(k):
        t_in(k, 0, half - 1)
        each(1, half, lambda d: t_fwd(k, d).start())

    def prepare(k):
        t_in(k, 1, half)
        for q in range(wide):
            tf[q * own:(q + 1) * own, :] = tg[k, q]
        hi, lo = split(tf[...])
        ts[k] = hi
        tt[k] = jnp.concatenate([hi, lo], axis=0).T

    def products(work):
        highs, lows = [None] * len(work), [None] * len(work)

        def stream(i, c):
            k, view = work[i]
            hi, _ = split(view[:, c:c + tile])
            p = lax.dot_general(hi, tt[k, c:c + tile, :], NN, preferred_element_type=F32)
            highs[i] = p if c == 0 else highs[i] + p

        def push(i, c):
            k, view = work[i]
            _, lo = split(view[:, c:c + tile])
            q = lax.dot_general(ts[k, :, c:c + tile], lo, NT, preferred_element_type=F32)
            lows[i] = q if c == 0 else lows[i] + q

        for c in range(0, cols, tile):
            for i in range(len(work)):
                push(i, c)
                stream(i, c)
        return highs, lows

    def reducer(az, aw, sems):
        def z_out(d):
            return remote(az.at[n], az.at[n], sems.at[0], sems.at[1], (w, zpeer(d)))

        def w_out(d):
            return remote(aw.at[w], aw.at[w], sems.at[2], sems.at[3], (lax.rem(w + d, wide), n))

        some_z = az.at[pl.ds(0, narrow - 1)]
        some_w = aw.at[pl.ds(0, wide - 1)]
        all_z = remote(some_z, some_z, sems.at[0], sems.at[1], (sib, n))
        all_w = remote(some_w, some_w, sems.at[2], sems.at[3], (sib, n))

        def z_start():
            for d in range(1, narrow):
                z_out(d).start()

        def z_finish():
            all_z.wait_recv()
            t = az[0]
            for q in range(1, narrow):
                t = t + az[q]
            aw[w] = t
            each(1, wide, lambda d: w_out(d).start())

        def w_finish():
            all_w.wait_recv()
            t = aw[0]
            for q in range(1, wide):
                t = t + aw[q]
            return t

        def drain():
            all_z.wait_send()
            all_w.wait_send()

        return z_start, z_finish, w_finish, drain

    c_start, c_mid, c_end, c_drain = reducer(azc, awc, c_sem)
    s_start, s_mid, s_end, s_drain = reducer(azs, aws, s_sem)
    c_start()
    forward(0)
    prepare(0)

    def advance(k, lo, hi):
        if lo == 0:
            load(k).wait()
        highs, lows = products([(k, buf.at[k % depth, j]) for j in range(lo, hi)])
        for j, p, q in zip(range(lo, hi), highs, lows):
            acc[j] = p if k == 0 else acc[j] + p
            low[j] = q if k == 0 else low[j] + q
        if k + depth < terms and hi == away:
            fetch(k + depth)

    def halves(k):
        advance(k, 0, 1)
        if k + 1 < terms:
            forward(k + 1)
        if away > 1:
            advance(k, 1, away)

    for k in range(terms):
        if k == 0:
            halves(0)
        else:
            prepare(k)
            if k == 1:
                halves(1)
            else:
                advance(k, 0, away)
        if k + depth >= terms:
            q = (k + depth - terms) * away
            for i in range(q, min(q + away, terms)):
                load_own(i).start()
        if k and k + 2 < terms:
            forward(k + 2)
        if k == 1:
            c_mid()

    def r_out(j):
        return remote(part.at[j], img.at[n], r_send, r_recv, (w, block(j)))

    some_img = img.at[pl.ds(0, away)]
    all_r = remote(part, some_img, r_send, r_recv, (sib, n))

    def settle(high, lows):
        v = high.T
        return v[0:ranks] + v[ranks:2 * ranks] + lows

    for j in range(away):
        part[j] = settle(acc[j], low[j])
        r_out(j).start()

    corr = unpack(c_end(), fold(m, m))
    eye = jnp.where(lax.broadcasted_iota(jnp.int32, (m, m), 0) == lax.broadcasted_iota(jnp.int32, (m, m), 1), 1.0, 0.0)
    e = corr - eye
    e2 = nn(e, e)
    out_hm[0] = eye - e
    out_hm[1] = (eye - e) + (e2 - nn(e, e2))

    high, lows = None, None
    for g in range(terms // group):
        for k in range(g * group, g * group + group):
            load_own(k).wait()
        ps, qs = products([(k, own_view(k)) for k in range(g * group, g * group + group)])
        p, q = functools.reduce(jnp.add, ps), functools.reduce(jnp.add, qs)
        high = p if g == 0 else high + p
        lows = q if g == 0 else lows + q

    image = settle(high, lows)
    all_r.wait_recv()
    for d in range(1, narrow):
        image = image + img[zpeer(d)]
    out_image[...] = image
    me = me_ref[...]
    both = nt(image, jnp.concatenate([me, image], axis=0))
    azs[n] = pack(both, fold(ranks, m + ranks))
    s_start()
    c_drain()
    all_r.wait_send()
    sent = tg.at[:, pl.ds(0, wide - 1)]
    remote(sent, sent, t_send, t_recv.at[0, 0], (sib, n)).wait_send()
    s_mid()
    out_sums[...] = s_end()
    s_drain()


def finish(total, image, sums, hm, me, new_out, proj_out, fac_out, new, proj, fac, sem):
    m = me.shape[0]
    ranks = image.shape[0]
    both = unpack(sums[...], fold(ranks, m + ranks))
    first_t = both[:, 0:m]
    square = both[:, m:m + ranks]
    proj_t = nn(first_t, hm[0])
    gram = (square - nt(nn(first_t, hm[1]), first_t)) * (1.0 / total)
    proj[...] = nt(hm[0], first_t)
    x, lower = factor_solve(gram, image[...] - nn(proj_t, me[...]))
    new[...] = x
    fac[...] = lower
    outs = [pltpu.make_async_copy(s, d, sem.at[i]) for i, (s, d) in enumerate(
        ((new, new_out), (proj, proj_out), (fac, fac_out)))]
    for c in outs:
        c.start()
    for c in outs:
        c.wait()


def body(wide, narrow, total, coefficients, tensor_blocks, basis_rows):
    terms, own, cols = tensor_blocks.shape
    m, rows = basis_rows.shape
    ranks = own * wide
    depth = min(DEPTH, terms)
    dma = lambda *s: pltpu.SemaphoreType.DMA(s)
    vm = lambda s, t=F32: pltpu.VMEM(s, t)
    shape = lambda *s: jax.ShapeDtypeStruct(s, F32)
    anywhere = pl.BlockSpec(memory_space=pl.ANY)
    inside = pl.BlockSpec(memory_space=pltpu.VMEM)
    cpack, spack = packed(m, m), packed(ranks, m + ranks)
    image, sums, hm = pl.pallas_call(
        functools.partial(kernel, wide, narrow),
        out_shape=(shape(ranks, rows), shape(*spack), shape(2, m, m)),
        in_specs=[pl.BlockSpec(memory_space=pltpu.HBM)] * 3,
        out_specs=[inside] * 3,
        scratch_shapes=[
            vm((depth, narrow - 1, rows, cols)),
            vm((terms, wide, own, cols)),
            vm((ranks, cols)),
            vm((terms, ranks, cols), BF16),
            vm((terms, cols, 2 * ranks), BF16),
            vm((narrow - 1, rows, 2 * ranks)),
            vm((narrow - 1, ranks, rows)),
            vm((m, rows)),
            vm((narrow - 1, ranks, rows)),
            vm((narrow, ranks, rows)),
            vm((narrow,) + cpack),
            vm((wide,) + cpack),
            vm((narrow,) + spack),
            vm((wide,) + spack),
            dma(depth), dma(terms), dma(2),
            pltpu.SemaphoreType.DMA, dma(terms, 2),
            pltpu.SemaphoreType.DMA, pltpu.SemaphoreType.DMA, dma(4), dma(4),
        ],
        compiler_params=pltpu.CompilerParams(
            collective_id=0, has_side_effects=True, vmem_limit_bytes=48 * 1024 * 1024),
        name="krylov_step",
    )(*[pltpu.with_memory_space_constraint(x, pltpu.HBM) for x in (coefficients, tensor_blocks, basis_rows)])
    return pl.pallas_call(
        functools.partial(finish, total),
        out_shape=(shape(ranks, rows), shape(m, ranks), shape(ranks, ranks)),
        in_specs=[inside] * 4,
        out_specs=[anywhere] * 3,
        scratch_shapes=[
            vm((ranks, rows)), vm((m, ranks)), vm((ranks, ranks)), dma(3),
        ],
        compiler_params=pltpu.CompilerParams(vmem_limit_bytes=4 * 1024 * 1024),
        name="krylov_finish",
    )(image, sums, hm, basis_rows)


def solution(mesh):
    wide, narrow = mesh.shape["wide"], mesh.shape["narrow"]
    in_specs = (P(None, "wide", "narrow"), P(None, "wide", "narrow"), P(None, ("wide", "narrow")))
    out_specs = (P(None, ("wide", "narrow")), P(), P())

    def whole(coefficients, tensor_blocks, basis_rows):
        total = coefficients.shape[1]
        return jax.shard_map(functools.partial(body, wide, narrow, total), mesh=mesh,
                             in_specs=in_specs, out_specs=out_specs, check_vma=False)(
            coefficients, tensor_blocks, basis_rows)

    return whole
```
